256 devices in a mesh: batch: 2 (over y_lo), space: 64 (over x, y_hi, z), hidden: 2 (over core).
Axes of the slice: x: 4, y: 4 (y_hi: 2, y_lo: 2; y = y_hi * 2 + y_lo), z: 8, core: 2. Of those that a mesh axis runs over, the one named last changes fastest.
Arguments:
- nodes: bfloat16 [2, 8192, 512], P('batch', 'space'), may hold values from -6 to 6
- edges: bfloat16 [2, 65536, 512], P('batch', 'space'), may hold values from -6 to 6
- node_cotangent: bfloat16 [2, 8192, 512], P('batch', 'space'), may hold values from -18 to 18
- edge_cotangent: bfloat16 [2, 65536, 512], P('batch', 'space'), may hold values from -18 to 18
- senders: int32 [65536], P('space'), may hold values from 0 to 255
- receivers: int32 [65536], P('space'), may hold values from 0 to 127
- send_lists: int32 [64, 2, 64], P('space'), may hold values from 0 to 127
- edge_first: bfloat16 [1536, 512], P(None, 'hidden'), may hold values from -0.15625 to 0.15625
- edge_bias: float32 [512], P('hidden'), may hold values from -3 to 3
- edge_second: bfloat16 [512, 512], P('hidden'), may hold values from -0.25 to 0.25
- edge_gain: float32 [512], replicated, may hold values from 0.1 to 1.9
- node_first: bfloat16 [1024, 512], replicated, may hold values from -0.1875 to 0.1875
- node_bias: float32 [512], replicated, may hold values from -3 to 3
- node_second: bfloat16 [512, 512], replicated, may hold values from -0.25 to 0.25
- node_gain: float32 [512], replicated, may hold values from 0.1 to 1.9
Outputs:
- grad_nodes: bfloat16 [2, 8192, 512], P('batch', 'space', 'hidden')
- grad_edges: bfloat16 [2, 65536, 512], P('batch', 'space', 'hidden')
- grad_edge_first: float32 [1536, 512], P(None, 'hidden')
- grad_edge_bias: float32 [512], P('hidden')
- grad_edge_second: float32 [512, 512], P('hidden')
- grad_edge_gain: float32 [512], replicated
- grad_node_first: float32 [1024, 512], replicated
- grad_node_bias: float32 [512], replicated
- grad_node_second: float32 [512, 512], replicated
- grad_node_gain: float32 [512], replicated
The draws below stay inside these ranges and needn't reach their ends.
Inputs may be any that keep to these rules, and one draw needn't show every extreme that they name: `senders`: an entry below 128 is a local node of the edge's patch; 128 + k is row k of the previous patch's list 1, 192 + k row k of the next patch's list 0. `receivers`: local nodes of the edge's patch. `send_lists`: local nodes of the patch; entries may repeat.
All inputs are finite; a program needn't handle non-finite values.
Results may differ from the reference program's by a relative error of at most 0.015.
Values may be sent and summed in bfloat16 or wider, within the bound.
A program may use at most 128 MiB of HBM per device.

```python
import jax
import jax.numpy as jnp
from jax import lax

D = 512
FF = 512
NODE_DEV = 128
HALO = 64
EDGE_DEV = 1024
TAB = 256
PATCHES = 64
NODES = 8192
EDGES = 65536
SAMPLES = 2


def rising_rows(key, row_count, width):
    first_key = jax.random.fold_in(key, 0)
    ramp = 1.0 + 2.0 * jnp.arange(row_count, dtype=jnp.float32) / row_count
    base = jnp.clip(jax.random.normal(first_key, (SAMPLES, row_count, width), jnp.float32), -6.0, 6.0)
    return base * ramp[None, :, None]


def draw_node_cotangent(key, part):
    return rising_rows(jax.random.fold_in(key, 7), NODES, D).astype(jnp.bfloat16)


def draw_edge_cotangent(key, part):
    return rising_rows(jax.random.fold_in(key, 11), EDGES, D).astype(jnp.bfloat16)


def plant(values, own_key, least, largest):
    spot = [jax.random.randint(jax.random.fold_in(own_key, axis), (), 0, length) for axis, length in enumerate(values.shape)]
    widest = values.shape.index(max(values.shape))
    neighbour = spot[:widest] + [(spot[widest] + 1) % values.shape[widest]] + spot[widest + 1:]
    return values.at[tuple(spot)].set(least).at[tuple(neighbour)].set(largest)


def levels(own_key, dims, cuts, low, top_value):
    level, own = 1.0, jax.random.fold_in(own_key, 6)
    for position, shards_of in cuts:
        steps = jnp.exp(jax.random.uniform(jax.random.fold_in(own, position), (shards_of,), jnp.float32, low / len(cuts), top_value / len(cuts)))
        level = level * jnp.repeat(steps, dims[position] // shards_of).reshape([-1 if axis == position else 1 for axis in range(len(dims))])
    return level


def normal_values(rng, dims, spread, most, pieces=(), held_as=jnp.bfloat16):
    drawn = spread * jax.random.normal(rng, dims, jnp.float32)
    if pieces:
        drawn = drawn * levels(rng, dims, pieces, -0.22, 0.18)
    return jnp.clip(drawn, -most, most).astype(held_as)


def setup_inputs(seed: int = 0) -> dict:
    seeds = jax.random.split(jax.random.key(seed), 16)
    nodes = normal_values(seeds[0], (SAMPLES, NODES, D), 1.0, 6.0, ((0, 2), (1, 64)))
    edges = normal_values(seeds[1], (SAMPLES, EDGES, D), 1.0, 6.0, ((0, 2), (1, 64)))
    node_cotangent = draw_node_cotangent(jax.random.fold_in(seeds[15], 71), 0)
    edge_cotangent = draw_edge_cotangent(jax.random.fold_in(seeds[15], 71), 0)
    senders = plant(jax.random.randint(seeds[4], (EDGES,), 0, TAB), jax.random.fold_in(seeds[4], 1), 0, TAB - 1).astype(jnp.int32)
    receivers = plant(jax.random.randint(seeds[5], (EDGES,), 0, NODE_DEV), jax.random.fold_in(seeds[5], 1), 0, NODE_DEV - 1).astype(jnp.int32)
    send_lists = plant(jax.random.randint(seeds[6], (PATCHES, 2, HALO), 0, NODE_DEV), jax.random.fold_in(seeds[6], 1), 0, NODE_DEV - 1).astype(jnp.int32)
    edge_first = normal_values(seeds[7], (3 * D, FF), (3 * D) ** -0.5, 0.15625, ((1, 2),))
    edge_bias = normal_values(seeds[8], (FF,), 0.5, 3.0, ((0, 2),), jnp.float32)
    edge_second = normal_values(seeds[9], (FF, D), FF ** -0.5, 0.25, ((0, 2),))
    edge_gain = jnp.clip(1.0 + 0.18 * jax.random.normal(seeds[10], (D,), jnp.float32), 0.1, 1.9)
    node_first = normal_values(seeds[11], (2 * D, FF), (2 * D) ** -0.5, 0.1875)
    node_bias = normal_values(seeds[12], (FF,), 0.5, 3.0, (), jnp.float32)
    node_second = normal_values(seeds[13], (FF, D), FF ** -0.5, 0.25)
    node_gain = jnp.clip(1.0 + 0.18 * jax.random.normal(seeds[14], (D,), jnp.float32), 0.1, 1.9)
    return {"nodes": nodes, "edges": edges, "node_cotangent": node_cotangent, "edge_cotangent": edge_cotangent, "senders": senders, "receivers": receivers, "send_lists": send_lists, "edge_first": edge_first, "edge_bias": edge_bias, "edge_second": edge_second, "edge_gain": edge_gain, "node_first": node_first, "node_bias": node_bias, "node_second": node_second, "node_gain": node_gain}


EPS = 1e-05

def matmul(lefthand, righthand):
    return jnp.dot(lefthand, righthand, preferred_element_type=jnp.float32)

def matmul_tn(lefthand, righthand):
    return lax.dot_general(lefthand, righthand, (((0,), (0,)), ((), ())), preferred_element_type=jnp.float32)

def matmul_nt(lefthand, righthand):
    return lax.dot_general(lefthand, righthand, (((1,), (1,)), ((), ())), preferred_element_type=jnp.float32)

def normalize(values):
    centre = values - lax.optimization_barrier(jnp.mean(values, axis=-1, keepdims=True))
    scaled = lax.rsqrt(lax.optimization_barrier(jnp.mean(centre * centre, axis=-1, keepdims=True)) + EPS)
    return (centre * scaled, scaled)

def norm_back(upstream, gain_vec, normed, scaled):
    pulled = upstream * gain_vec
    return scaled * (pulled - lax.optimization_barrier(jnp.mean(pulled, axis=-1, keepdims=True)) - normed * lax.optimization_barrier(jnp.mean(pulled * normed, axis=-1, keepdims=True)))

def silu_slope(values):
    logistic = jax.nn.sigmoid(values)
    return logistic * (1.0 + values * (1.0 - logistic))

def reference(nodes, edges, node_cotangent, edge_cotangent, senders, receivers, send_lists, edge_first, edge_bias, edge_second, edge_gain, node_first, node_bias, node_second, node_gain):
    samples = nodes.shape[0]
    patch_ids = jnp.arange(PATCHES, dtype=jnp.int32)[:, None]
    sample_ids = jnp.arange(samples, dtype=jnp.int32)[:, None]
    node_blocks = nodes.reshape(samples, PATCHES, NODE_DEV, D)
    send_ids = senders.reshape(PATCHES, EDGE_DEV)
    recv_ids = receivers.reshape(PATCHES, EDGE_DEV)
    to_prev = node_blocks[:, patch_ids, send_lists[:, 0, :]]
    to_next = node_blocks[:, patch_ids, send_lists[:, 1, :]]
    table = jnp.concatenate([node_blocks, jnp.roll(to_next, 1, axis=1), jnp.roll(to_prev, -1, axis=1)], axis=2)
    from_sender = table[:, patch_ids, send_ids]
    from_receiver = node_blocks[:, patch_ids, recv_ids]
    edge_blocks = edges.reshape(samples, PATCHES, EDGE_DEV, D)
    edge_input = jnp.concatenate([edge_blocks, from_sender, from_receiver], axis=3).reshape(-1, 3 * D)
    edge_pre = matmul(edge_input, edge_first) + edge_bias
    edge_act = jax.nn.silu(edge_pre).astype(jnp.bfloat16)
    edge_normed, edge_scale = normalize(matmul(edge_act, edge_second))
    message = (edge_gain * edge_normed).astype(jnp.bfloat16)
    flat_recv = (patch_ids * NODE_DEV + recv_ids).reshape(-1)
    segment_ids = (sample_ids * NODES + flat_recv[None, :]).reshape(-1)
    gathered = jax.ops.segment_sum(message.astype(jnp.float32), segment_ids, num_segments=samples * NODES).astype(jnp.bfloat16)
    node_input = jnp.concatenate([nodes.reshape(-1, D), gathered], axis=1)
    node_pre = matmul(node_input, node_first) + node_bias
    node_act = jax.nn.silu(node_pre).astype(jnp.bfloat16)
    node_normed, node_scale = normalize(matmul(node_act, node_second))
    node_upstream = node_cotangent.reshape(-1, D).astype(jnp.float32)
    grad_node_gain = lax.optimization_barrier(jnp.sum(node_upstream * node_normed, axis=0))
    node_dz = norm_back(node_upstream, node_gain, node_normed, node_scale).astype(jnp.bfloat16)
    grad_node_second = matmul_tn(node_act, node_dz)
    node_dh = (matmul_nt(node_dz, node_second) * silu_slope(node_pre)).astype(jnp.bfloat16)
    grad_node_first = matmul_tn(node_input, node_dh)
    grad_node_bias = lax.optimization_barrier(jnp.sum(node_dh.astype(jnp.float32), axis=0))
    node_dx = matmul_nt(node_dh, node_first)
    agg_grad = node_dx[:, D:].astype(jnp.bfloat16)
    edge_upstream = edge_cotangent.reshape(-1, D).astype(jnp.float32)
    message_grad = edge_upstream + agg_grad[segment_ids].astype(jnp.float32)
    grad_edge_gain = lax.optimization_barrier(jnp.sum(message_grad * edge_normed, axis=0))
    edge_dz = norm_back(message_grad, edge_gain, edge_normed, edge_scale).astype(jnp.bfloat16)
    grad_edge_second = matmul_tn(edge_act, edge_dz)
    edge_dh = (matmul_nt(edge_dz, edge_second) * silu_slope(edge_pre)).astype(jnp.bfloat16)
    grad_edge_first = matmul_tn(edge_input, edge_dh)
    grad_edge_bias = lax.optimization_barrier(jnp.sum(edge_dh.astype(jnp.float32), axis=0))
    edge_part = matmul_nt(edge_dh, edge_first[:D])
    grad_edges = (edge_upstream + edge_part).astype(jnp.bfloat16).reshape(samples, EDGES, D)
    send_part = matmul_nt(edge_dh, edge_first[D:2 * D])
    table_ids = (sample_ids * (PATCHES * TAB) + (patch_ids * TAB + send_ids).reshape(-1)[None, :]).reshape(-1)
    table_grad = jax.ops.segment_sum(send_part, table_ids, num_segments=samples * PATCHES * TAB).reshape(samples, PATCHES, TAB, D)
    recv_part = matmul_nt(edge_dh, edge_first[2 * D:])
    recv_grad = jax.ops.segment_sum(recv_part, segment_ids, num_segments=samples * NODES).reshape(samples, PATCHES, NODE_DEV, D)
    own_grad = table_grad[:, :, :NODE_DEV] + recv_grad
    back_prev = jnp.roll(table_grad[:, :, NODE_DEV + HALO:], 1, axis=1)
    back_next = jnp.roll(table_grad[:, :, NODE_DEV:NODE_DEV + HALO], -1, axis=1)
    own_grad = own_grad.at[:, patch_ids, send_lists[:, 0, :]].add(back_prev)
    own_grad = own_grad.at[:, patch_ids, send_lists[:, 1, :]].add(back_next)
    grad_nodes = (node_upstream + node_dx[:, :D] + own_grad.reshape(-1, D)).astype(jnp.bfloat16).reshape(samples, NODES, D)
    return (grad_nodes, grad_edges, grad_edge_first, grad_edge_bias, grad_edge_second, grad_edge_gain, grad_node_first, grad_node_bias, grad_node_second, grad_node_gain)
```

```python
import jax
import jax.numpy as jnp
from jax import lax
from jax.experimental import pallas as pl
from jax.experimental.pallas import tpu as pltpu
from jax.sharding import PartitionSpec as P

EPS = 1e-05


def extended(cells, sides, width):
    for axis, dim in sides:
        count = lax.axis_size(axis)
        head = lax.slice_in_dim(cells, 0, width, axis=dim)
        tail = lax.slice_in_dim(cells, cells.shape[dim] - width, cells.shape[dim], axis=dim)
        cells = jnp.concatenate(
            [
                lax.ppermute(tail, axis, [(i, (i + 1) % count) for i in range(count)]),
                cells,
                lax.ppermute(head, axis, [((i + 1) % count, i) for i in range(count)]),
            ],
            axis=dim,
        )
    return cells


def copy_for_each(value, axis):
    devices = lax.axis_size(axis)
    return lax.all_to_all(
        jnp.broadcast_to(value[None], (devices, *value.shape)), axis, 0, 0, tiled=True
    )


def taken_together(value, axis):
    return copy_for_each(value, axis).astype(jnp.float32).sum(axis=0)


def cut_along(value, dim, devices):
    lengths = value.shape
    pieces = value.reshape(*lengths[:dim], devices, lengths[dim] // devices, *lengths[dim + 1 :])
    return jnp.moveaxis(pieces, dim, 0)


def sent_and_summed(value, axis, dim):
    devices = lax.axis_size(axis)
    pieces = lax.all_to_all(cut_along(value, dim, devices), axis, 0, 0, tiled=True)
    return jnp.sum(pieces.astype(jnp.float32), axis=0)


def in_one_piece(arrays, axis, dim, along):
    ends, at = ([], 0)
    for a in arrays[:-1]:
        at += a.shape[along]
        ends.append(at)
    both = jnp.concatenate(arrays, axis=along)
    return tuple(jnp.split(sent_and_summed(both, axis, dim), ends, axis=along))


def in_one(arrays, axis):
    ends = [0]
    for a in arrays:
        ends.append(ends[-1] + a.size)
    so_far = lax.psum(jnp.concatenate([a.ravel() for a in arrays]), axis)
    return tuple((so_far[b:e].reshape(a.shape) for a, b, e in zip(arrays, ends, ends[1:])))


def one_hot(indices, columns, wanted):
    return (indices[:, None] == jnp.arange(columns, dtype=jnp.int32)[None, :]).astype(wanted)


def matmul(lefthand, righthand):
    return jnp.dot(lefthand, righthand, preferred_element_type=jnp.float32)


def matmul_tn(lefthand, righthand):
    return lax.dot_general(
        lefthand, righthand, (((0,), (0,)), ((), ())), preferred_element_type=jnp.float32
    )


def matmul_nt(lefthand, righthand):
    return lax.dot_general(
        lefthand, righthand, (((1,), (1,)), ((), ())), preferred_element_type=jnp.float32
    )


def exact_tn(lefthand, righthand):
    return lax.dot_general(
        lefthand,
        righthand,
        (((0,), (0,)), ((), ())),
        precision=lax.Precision.HIGHEST,
        preferred_element_type=jnp.float32,
    )


def normalize(values):
    centre = values - jnp.mean(values, axis=-1, keepdims=True)
    scaled = lax.rsqrt(jnp.mean(centre * centre, axis=-1, keepdims=True) + EPS)
    return (centre * scaled, scaled)


def norm_back(upstream, gain_vec, normed, scaled):
    pulled = upstream * gain_vec
    return scaled * (
        pulled
        - jnp.mean(pulled, axis=-1, keepdims=True)
        - normed * jnp.mean(pulled * normed, axis=-1, keepdims=True)
    )


def silu_slope(values):
    logistic = jax.nn.sigmoid(values)
    return logistic * (1.0 + values * (1.0 - logistic))


ROWS = 2048
COLOR = ROWS // 2
WIDE = COLOR // 4
NARROW = WIDE // 4
ZROWS = 2 * NARROW // 8
NODE_ROWS = 768
NODE_AT = 1024
MESH = pl.DeviceIdType.MESH


def rows_at(ref, start, count):
    return ref.at[pl.ds(pl.multiple_of(start, 16), count)]


def load_rows(ref, start, count):
    return ref[pl.ds(pl.multiple_of(start, 16), count), :].astype(jnp.float32)


def remote(src, dst, sems, k, device):
    return pltpu.make_async_remote_copy(
        src_ref=src,
        dst_ref=dst,
        send_sem=sems.at[0, k],
        recv_sem=sems.at[1, k],
        device_id=device,
        device_id_type=MESH,
    )


def scatter_start(src, base, n, d, ahead, behind, held, sems):
    h = n // 2
    far, up, down = (base + lax.rem(d + k, 4) * n for k in (2, 1, 3))
    copies = [
        remote(rows_at(src, far, h), held.at[0], sems, 0, ahead),
        remote(rows_at(src, far + h, h), held.at[1], sems, 1, behind),
        remote(rows_at(src, up + h, h), held.at[2], sems, 2, ahead),
        remote(rows_at(src, down, h), held.at[3], sems, 3, behind),
    ]
    for c in copies:
        c.start()
    return copies


def scatter_middle(src, base, n, d, ahead, behind, held, made, sems, copies):
    h = n // 2
    up, down = (base + lax.rem(d + k, 4) * n for k in (1, 3))
    copies[0].wait_recv()
    made[0] = (load_rows(src, up, h) + held[0].astype(jnp.float32)).astype(jnp.bfloat16)
    c = remote(made.at[0], held.at[4], sems, 4, ahead)
    c.start()
    copies.append(c)
    copies[1].wait_recv()
    made[1] = (load_rows(src, down + h, h) + held[1].astype(jnp.float32)).astype(jnp.bfloat16)
    c = remote(made.at[1], held.at[5], sems, 5, behind)
    c.start()
    copies.append(c)


def scatter_end(src, base, n, d, held, dst, at, copies):
    h = n // 2
    own = base + d * n
    for k in (3, 4):
        copies[k].wait_recv()
    dst[pl.ds(at, h), :] = (
        load_rows(src, own, h) + held[3].astype(jnp.float32) + held[4].astype(jnp.float32)
    ).astype(jnp.bfloat16)
    for k in (2, 5):
        copies[k].wait_recv()
    dst[pl.ds(at + h, h), :] = (
        load_rows(src, own + h, h) + held[2].astype(jnp.float32) + held[5].astype(jnp.float32)
    ).astype(jnp.bfloat16)
    for c in copies:
        c.wait_send()


def gather_start(out, base, n, d, ahead, behind, sems):
    h = n // 2
    own = base + d * n
    copies = []
    for k, (at, device) in enumerate(
        ((own, ahead), (own + h, behind), (own + h, ahead), (own, behind))
    ):
        c = remote(rows_at(out, at, h), rows_at(out, at, h), sems, k, device)
        c.start()
        copies.append(c)
    return copies


def gather_middle(out, base, n, d, ahead, behind, sems, copies):
    h = n // 2
    up, down = (base + lax.rem(d + k, 4) * n for k in (1, 3))
    for k, (j, at, device) in enumerate(((0, down, ahead), (1, up + h, behind))):
        copies[j].wait_recv()
        c = remote(rows_at(out, at, h), rows_at(out, at, h), sems, 4 + k, device)
        c.start()
        copies.append(c)


def gather_end(copies):
    for c in copies[2:]:
        c.wait_recv()
    for c in copies:
        c.wait_send()


def reduce_kernel(
    g,
    out,
    other,
    held_wide,
    made_wide,
    kept_wide,
    held_narrow,
    made_narrow,
    kept_narrow,
    held_z,
    sems_wide,
    sems_narrow,
    sems_z,
    sems_out_z,
    sems_out_narrow,
    sems_out_wide,
    sems_core,
):
    batch = lax.axis_index("batch")
    space = lax.axis_index("space")
    core = lax.axis_index("hidden")
    x = space // 16
    y = (space // 8) % 2 * 2 + batch
    z = space % 8

    def device(i, j, k):
        return (j % 2, (i * 2 + j // 2) * 8 + k, core)

    x_up, x_down = (device((x + k) % 4, y, z) for k in (1, 3))
    y_up, y_down = (device(x, (y + k) % 4, z) for k in (1, 3))
    z_peers = [device(x, y, (z + k) % 8) for k in range(1, 8)]
    partner = (batch, space, 1 - core)
    barrier = pltpu.get_barrier_semaphore()
    peers = [x_up, x_down, y_up, y_down, *z_peers, partner]
    for peer in peers:
        pl.semaphore_signal(barrier, inc=1, device_id=peer, device_id_type=MESH)
    pl.semaphore_wait(barrier, len(peers))

    along = ((x, x_up, x_down), (y, y_up, y_down))
    started = []
    for color in (0, 1):
        pos, ahead, behind = along[color]
        started.append(
            scatter_start(
                g, color * COLOR, WIDE, pos, ahead, behind, held_wide.at[color], sems_wide.at[color]
            )
        )
    for color in (0, 1):
        pos, ahead, behind = along[color]
        scatter_middle(
            g, color * COLOR, WIDE, pos, ahead, behind, held_wide.at[color],
            made_wide.at[color], sems_wide.at[color], started[color],
        )
    second = []
    for color in (0, 1):
        pos, ahead, behind = along[color]
        scatter_end(
            g, color * COLOR, WIDE, pos, held_wide.at[color], kept_wide.at[color], 0, started[color]
        )
        pos, ahead, behind = along[1 - color]
        second.append(
            scatter_start(
                kept_wide.at[color], 0, NARROW, pos, ahead, behind,
                held_narrow.at[color], sems_narrow.at[color],
            )
        )
    for color in (0, 1):
        pos, ahead, behind = along[1 - color]
        scatter_middle(
            kept_wide.at[color], 0, NARROW, pos, ahead, behind, held_narrow.at[color],
            made_narrow.at[color], sems_narrow.at[color], second[color],
        )
    for color in (0, 1):
        pos, ahead, behind = along[1 - color]
        scatter_end(
            kept_wide.at[color], 0, NARROW, pos, held_narrow.at[color],
            kept_narrow, color * NARROW, second[color],
        )
    third = []
    for k in range(1, 8):
        c = remote(
            rows_at(kept_narrow, (z + k) % 8 * ZROWS, ZROWS), held_z.at[k - 1], sems_z, k - 1,
            z_peers[k - 1],
        )
        c.start()
        third.append(c)
    total = load_rows(kept_narrow, z * ZROWS, ZROWS)
    for k in range(7):
        third[k].wait_recv()
        total = total + held_z[k].astype(jnp.float32)
    base = (x * WIDE + y * NARROW, COLOR + y * WIDE + x * NARROW)
    upper = z // 4
    mine = (1 - upper) * base[0] + upper * base[1] + z % 4 * ZROWS
    out[pl.ds(pl.multiple_of(mine, 16), ZROWS), :] = total.astype(jnp.bfloat16)
    for c in third:
        c.wait_send()
    third = []
    for k in range(1, 8):
        c = remote(rows_at(out, mine, ZROWS), rows_at(out, mine, ZROWS), sems_out_z, k - 1, z_peers[k - 1])
        c.start()
        third.append(c)
    for c in third:
        c.wait_recv()
    for c in third:
        c.wait_send()
    bases = ((0 + x * WIDE), (COLOR + y * WIDE))
    copies = []
    for color in (0, 1):
        pos, ahead, behind = along[1 - color]
        copies.append(gather_start(out, bases[color], NARROW, pos, ahead, behind, sems_out_narrow.at[color]))
    for color in (0, 1):
        pos, ahead, behind = along[1 - color]
        gather_middle(out, bases[color], NARROW, pos, ahead, behind, sems_out_narrow.at[color], copies[color])
    wide = []
    for color in (0, 1):
        gather_end(copies[color])
        pos, ahead, behind = along[color]
        wide.append(gather_start(out, color * COLOR, WIDE, pos, ahead, behind, sems_out_wide.at[color]))
    for color in (0, 1):
        pos, ahead, behind = along[color]
        gather_middle(out, color * COLOR, WIDE, pos, ahead, behind, sems_out_wide.at[color], wide[color])
    for color in (1, 0):
        gather_end(wide[color])
        if color == 1:
            c = remote(out.at[pl.ds(NODE_AT, NODE_ROWS)], other, sems_core, 0, partner)
            c.start()
    c.wait()


def reduce_all(packed):
    dma = pltpu.SemaphoreType.DMA
    bf16 = jnp.bfloat16
    columns = packed.shape[1]
    vmem = pl.BlockSpec(memory_space=pltpu.VMEM)
    return pl.pallas_call(
        reduce_kernel,
        out_shape=(
            jax.ShapeDtypeStruct(packed.shape, bf16),
            jax.ShapeDtypeStruct((NODE_ROWS, columns), bf16),
        ),
        in_specs=[vmem],
        out_specs=(vmem, vmem),
        scratch_shapes=[
            pltpu.VMEM((2, 6, WIDE // 2, columns), bf16),
            pltpu.VMEM((2, 2, WIDE // 2, columns), bf16),
            pltpu.VMEM((2, WIDE, columns), bf16),
            pltpu.VMEM((2, 6, NARROW // 2, columns), bf16),
            pltpu.VMEM((2, 2, NARROW // 2, columns), bf16),
            pltpu.VMEM((2 * NARROW, columns), bf16),
            pltpu.VMEM((7, ZROWS, columns), bf16),
            dma((2, 2, 6)),
            dma((2, 2, 6)),
            dma((2, 7)),
            dma((2, 7)),
            dma((2, 2, 6)),
            dma((2, 2, 6)),
            dma((2, 1)),
        ],
        compiler_params=pltpu.CompilerParams(collective_id=1, has_side_effects=True),
        name="reduce_all",
    )(packed)


def halves_of(part, count, my_part):
    return lax.dynamic_slice_in_dim(part, my_part * count, count, 0)


def on_device(
    nodes,
    edges,
    node_cotangent,
    edge_cotangent,
    senders,
    receivers,
    send_lists,
    edge_first,
    edge_bias,
    edge_second,
    edge_gain,
    node_first,
    node_bias,
    node_second,
    node_gain,
):
    splits = lax.axis_size("hidden")
    my_part = lax.axis_index("hidden")
    width = nodes.shape[2]
    half = width // splits
    node_rows = nodes[0]
    node_count = node_rows.shape[0]
    halo_count = send_lists.shape[2]
    listed = send_lists[0].reshape(-1)
    picker = one_hot(listed, node_count, jnp.bfloat16)
    outgoing = matmul(picker, node_rows).astype(jnp.bfloat16).reshape(2, halo_count, width)
    padded = extended(outgoing, (("space", 0),), 1)
    table = jnp.concatenate([node_rows, padded[0], padded[3]], axis=0)
    table_rows = table.shape[0]
    sender_hot = one_hot(senders, table_rows, jnp.bfloat16)
    receiver_hot = one_hot(receivers, node_count, jnp.bfloat16)
    from_sender = matmul(sender_hot, table).astype(jnp.bfloat16)
    from_receiver = matmul(receiver_hot, node_rows).astype(jnp.bfloat16)
    edge_input = jnp.concatenate([edges[0], from_sender, from_receiver], axis=1)
    edge_pre = matmul(edge_input, edge_first) + edge_bias
    edge_act = jax.nn.silu(edge_pre).astype(jnp.bfloat16)
    edge_total = taken_together(
        matmul(edge_act, edge_second).astype(jnp.bfloat16), "hidden"
    ).astype(jnp.float32)
    edge_normed, edge_scale = normalize(edge_total)
    message = (edge_gain * edge_normed).astype(jnp.bfloat16)
    gathered = matmul_tn(receiver_hot, message).astype(jnp.bfloat16)
    node_input = jnp.concatenate([node_rows, gathered], axis=1)
    node_pre = matmul(node_input, node_first) + node_bias
    node_act = jax.nn.silu(node_pre).astype(jnp.bfloat16)
    node_normed, node_scale = normalize(matmul(node_act, node_second))
    node_upstream = node_cotangent[0].astype(jnp.float32)
    node_gain_grad = jnp.sum(node_upstream * node_normed, axis=0)
    node_dz = norm_back(node_upstream, node_gain, node_normed, node_scale).astype(jnp.bfloat16)
    node_second_grad = matmul_tn(node_act, node_dz)
    node_dh = (matmul_nt(node_dz, node_second) * silu_slope(node_pre)).astype(jnp.bfloat16)
    node_first_grad = matmul_tn(node_input, node_dh)
    node_bias_grad = jnp.sum(node_dh.astype(jnp.float32), axis=0)
    node_dx = matmul_nt(node_dh, node_first)
    agg_grad = node_dx[:, width:].astype(jnp.bfloat16)
    edge_upstream = edge_cotangent[0].astype(jnp.float32)
    message_grad = edge_upstream + matmul(receiver_hot, agg_grad)
    edge_gain_grad = jnp.sum(message_grad * edge_normed, axis=0)
    edge_dz = norm_back(message_grad, edge_gain, edge_normed, edge_scale).astype(jnp.bfloat16)
    edge_second_grad = matmul_tn(edge_act, edge_dz)
    edge_dh = (matmul_nt(edge_dz, edge_second) * silu_slope(edge_pre)).astype(jnp.bfloat16)
    edge_first_grad = matmul_tn(edge_input, edge_dh)
    edge_bias_grad = jnp.sum(edge_dh.astype(jnp.float32), axis=0)
    sender_exact = one_hot(senders, table_rows, jnp.float32)
    receiver_exact = one_hot(receivers, node_count, jnp.float32)
    partial_grad = matmul_nt(edge_dh, edge_first)
    sender_part = exact_tn(sender_exact, partial_grad[:, width : 2 * width])
    receiver_part = exact_tn(receiver_exact, partial_grad[:, 2 * width :])
    table_part = jnp.concatenate(
        [sender_part[:node_count] + receiver_part, sender_part[node_count:]], axis=0
    )
    edge_own, table_grad = in_one_piece(
        (partial_grad[:, :width].astype(jnp.bfloat16), table_part.astype(jnp.bfloat16)),
        "hidden",
        1,
        0,
    )
    returning = jnp.stack(
        [table_grad[node_count : node_count + halo_count], table_grad[node_count + halo_count :]],
        axis=0,
    )
    returned = extended(returning.astype(jnp.bfloat16), (("space", 0),), 1).astype(returning.dtype)
    arriving = jnp.concatenate([returned[0], returned[3]], axis=0)
    halo_grad = exact_tn(one_hot(listed, node_count, jnp.float32), arriving)
    own_cot = lax.dynamic_slice_in_dim(node_upstream, my_part * half, half, 1)
    own_node = lax.dynamic_slice_in_dim(node_dx, my_part * half, half, 1)
    grad_nodes = (own_cot + own_node + table_grad[:node_count] + halo_grad).astype(jnp.bfloat16)[
        None
    ]
    own_edge_cot = lax.dynamic_slice_in_dim(edge_upstream, my_part * half, half, 1)
    grad_edges = (own_edge_cot + edge_own).astype(jnp.bfloat16)[None]
    bf16 = jnp.bfloat16
    first_rows = edge_first_grad.shape[0] // 2
    small = jnp.stack(
        [
            jnp.concatenate([edge_bias_grad, edge_bias_grad]),
            edge_gain_grad,
            node_bias_grad,
            node_gain_grad,
        ]
    )
    packed = jnp.concatenate(
        [
            jnp.concatenate(
                [edge_first_grad[:first_rows], edge_first_grad[first_rows:]], axis=1
            ).astype(bf16),
            edge_second_grad.astype(bf16),
            halves_of(node_first_grad.astype(bf16), 512, my_part),
            halves_of(node_second_grad.astype(bf16), 256, my_part),
            jnp.pad(small, ((0, 252), (0, 0))).astype(bf16),
        ],
        axis=0,
    )
    summed, other = reduce_all(packed)
    f32 = jnp.float32
    edge_first_grad = jnp.concatenate(
        [summed[:first_rows, :256], summed[:first_rows, 256:]], axis=0
    ).astype(f32)
    edge_second_grad = summed[768:1024].astype(f32)
    own = summed[1024:1792]
    lower = jnp.where(my_part == 0, own, other)
    upper = jnp.where(my_part == 0, other, own)
    node_first_grad = jnp.concatenate([lower[:512], upper[:512]], axis=0).astype(f32)
    node_second_grad = jnp.concatenate([lower[512:], upper[512:]], axis=0).astype(f32)
    small = summed[1792:1796].astype(f32)
    edge_bias_grad = small[0, :256]
    edge_gain_grad, node_bias_grad, node_gain_grad = small[1], small[2], small[3]
    return (
        grad_nodes,
        grad_edges,
        edge_first_grad,
        edge_bias_grad,
        edge_second_grad,
        edge_gain_grad,
        node_first_grad,
        node_bias_grad,
        node_second_grad,
        node_gain_grad,
    )


def solution(mesh):
    placed = (
        P("batch", "space", None),
        P("batch", "space", None),
        P("batch", "space", None),
        P("batch", "space", None),
        P("space"),
        P("space"),
        P("space", None, None),
        P(None, "hidden"),
        P("hidden"),
        P("hidden", None),
        P(),
        P(),
        P(),
        P(),
        P(),
    )
    return jax.shard_map(
        on_device,
        mesh=mesh,
        in_specs=placed,
        out_specs=(
            P("batch", "space", "hidden"),
            P("batch", "space", "hidden"),
            P(None, "hidden"),
            P("hidden"),
            P("hidden", None),
            P(),
            P(),
            P(),
            P(),
            P(),
        ),
        check_vma=False,
    )
```

```python
import jax
import jax.numpy as jnp
from jax import lax
from jax.experimental import pallas as pl
from jax.experimental.pallas import tpu as pltpu
from jax.sharding import PartitionSpec as P

EPS = 1e-05


def hot_columns(indices, rows):
    wanted = lax.broadcasted_iota(jnp.int32, (rows, indices.shape[1]), 0)
    return jnp.where(wanted == indices, 1.0, 0.0).astype(jnp.bfloat16)


def nn(lefthand, righthand):
    return jnp.dot(lefthand, righthand, preferred_element_type=jnp.float32)


def tn(lefthand, righthand):
    return lax.dot_general(
        lefthand, righthand, (((0,), (0,)), ((), ())), preferred_element_type=jnp.float32
    )


def nt(lefthand, righthand):
    return lax.dot_general(
        lefthand, righthand, (((1,), (1,)), ((), ())), preferred_element_type=jnp.float32
    )


def normalize(values):
    centre = values - jnp.mean(values, axis=-1, keepdims=True)
    scaled = lax.rsqrt(jnp.mean(centre * centre, axis=-1, keepdims=True) + EPS)
    return (centre * scaled, scaled)


def norm_back(pulled, normed, scaled):
    return scaled * (
        pulled
        - jnp.mean(pulled, axis=-1, keepdims=True)
        - normed * jnp.mean(pulled * normed, axis=-1, keepdims=True)
    )


def silu(values):
    return values / (1.0 + jnp.exp(-values))


def silu_slope(values):
    logistic = 1.0 / (1.0 + jnp.exp(-values))
    return logistic * (1.0 + values * (1.0 - logistic))


ROWS = 2048
COLOR = ROWS // 2
WIDE = COLOR // 4
NARROW = WIDE // 4
ZROWS = 2 * NARROW // 8
NODE_ROWS = 784
NODE_AT = 1024
MESH = pl.DeviceIdType.MESH


def rows_at(ref, start, count):
    return ref.at[pl.ds(pl.multiple_of(start, 16), count)]


def load_rows(ref, start, count):
    return ref[pl.ds(pl.multiple_of(start, 16), count), :].astype(jnp.float32)


def remote(src, dst, sems, k, device):
    return pltpu.make_async_remote_copy(
        src_ref=src,
        dst_ref=dst,
        send_sem=sems.at[0, k],
        recv_sem=sems.at[1, k],
        device_id=device,
        device_id_type=MESH,
    )


def scatter_start(src, base, n, d, ahead, behind, held, sems):
    h = n // 2
    far, up, down = (base + lax.rem(d + k, 4) * n for k in (2, 1, 3))
    copies = [
        remote(rows_at(src, far, h), held.at[0], sems, 0, ahead),
        remote(rows_at(src, far + h, h), held.at[1], sems, 1, behind),
        remote(rows_at(src, up + h, h), held.at[2], sems, 2, ahead),
        remote(rows_at(src, down, h), held.at[3], sems, 3, behind),
    ]
    for c in copies:
        c.start()
    return copies


def scatter_middle(src, base, n, d, ahead, behind, held, made, sems, copies):
    h = n // 2
    up, down = (base + lax.rem(d + k, 4) * n for k in (1, 3))
    copies[0].wait_recv()
    made[0] = (load_rows(src, up, h) + held[0].astype(jnp.float32)).astype(jnp.bfloat16)
    c = remote(made.at[0], held.at[4], sems, 4, ahead)
    c.start()
    copies.append(c)
    copies[1].wait_recv()
    made[1] = (load_rows(src, down + h, h) + held[1].astype(jnp.float32)).astype(jnp.bfloat16)
    c = remote(made.at[1], held.at[5], sems, 5, behind)
    c.start()
    copies.append(c)


def scatter_end(src, base, n, d, held, dst, at, copies):
    h = n // 2
    own = base + d * n
    for k in (3, 4):
        copies[k].wait_recv()
    dst[pl.ds(at, h), :] = (
        load_rows(src, own, h) + held[3].astype(jnp.float32) + held[4].astype(jnp.float32)
    ).astype(jnp.bfloat16)
    for k in (2, 5):
        copies[k].wait_recv()
    dst[pl.ds(at + h, h), :] = (
        load_rows(src, own + h, h) + held[2].astype(jnp.float32) + held[5].astype(jnp.float32)
    ).astype(jnp.bfloat16)
    for c in copies:
        c.wait_send()


def gather_start(out, base, n, d, ahead, behind, sems):
    h = n // 2
    own = base + d * n
    copies = []
    for k, (at, device) in enumerate(
        ((own, ahead), (own + h, behind), (own + h, ahead), (own, behind))
    ):
        c = remote(rows_at(out, at, h), rows_at(out, at, h), sems, k, device)
        c.start()
        copies.append(c)
    return copies


def gather_middle(out, base, n, d, ahead, behind, sems, copies):
    h = n // 2
    up, down = (base + lax.rem(d + k, 4) * n for k in (1, 3))
    for k, (j, at, device) in enumerate(((0, down, ahead), (1, up + h, behind))):
        copies[j].wait_recv()
        c = remote(rows_at(out, at, h), rows_at(out, at, h), sems, 4 + k, device)
        c.start()
        copies.append(c)


def gather_end(copies):
    for c in copies[2:]:
        c.wait_recv()
    for c in copies:
        c.wait_send()


EDGES = 1024
NODES = 128
HALO = 64
WIDTH = 512
HALF = 256
TILE = 256
TILES = EDGES // TILE


def places():
    batch = lax.axis_index("batch")
    space = lax.axis_index("space")
    core = lax.axis_index("hidden")
    return (
        core,
        (batch, space, 1 - core),
        (batch, (space + 63) % 64, core),
        (batch, (space + 1) % 64, core),
    )


def layer_kernel(
    nodes,
    listed,
    senders,
    receivers,
    first,
    second,
    edge_bias,
    edge_gain,
    node_bias,
    node_gain,
    edges_far,
    cot_far,
    node_cot_far,
    node_first_far,
    node_second_far,
    g,
    edge_mine,
    edge_send,
    table_mine,
    table_send,
    edges,
    cot,
    node_cot,
    node_first,
    node_second,
    other_first,
    other_second,
    other_bias,
    outgoing,
    table,
    hot,
    pre,
    lifted,
    act,
    normed,
    scale,
    agg,
    node_input,
    node_act,
    agg_grad,
    dz,
    dh,
    sums,
    local_sems,
    sems,
):
    bf16, f32 = jnp.bfloat16, jnp.float32
    core, partner, before, after = places()
    barrier = pltpu.get_barrier_semaphore()
    for peer in (partner, before, after):
        pl.semaphore_signal(barrier, inc=1, device_id=peer, device_id_type=MESH)
    loads = [
        pltpu.make_async_copy(src, dst, local_sems.at[k])
        for k, (src, dst) in enumerate(
            (
                (edges_far, edges),
                (node_first_far, node_first),
                (node_second_far, node_second),
                (node_cot_far, node_cot),
                (cot_far, cot),
            )
        )
    ]
    for c in loads:
        c.start()
    outgoing[...] = tn(hot_columns(listed[...], NODES), nodes[...]).astype(bf16)
    table[0:NODES] = nodes[...]
    pl.semaphore_wait(barrier, 3)
    sent = [
        remote(first, other_first, sems, 0, partner),
        remote(edge_bias, other_bias, sems, 1, partner),
        remote(second, other_second, sems, 2, partner),
        remote(outgoing.at[pl.ds(0, HALO)], table.at[pl.ds(NODES + HALO, HALO)], sems, 3, before),
        remote(outgoing.at[pl.ds(HALO, HALO)], table.at[pl.ds(NODES, HALO)], sems, 4, after),
    ]
    for c in (sent[3], sent[4], sent[0], sent[1], sent[2]):
        c.start()
    for t in range(TILES):
        hot[t, 0 : 2 * NODES] = hot_columns(senders[:, t * TILE : (t + 1) * TILE], 2 * NODES)
        hot[t, 2 * NODES :] = hot_columns(receivers[:, t * TILE : (t + 1) * TILE], NODES)

    def lift(weights, columns):
        for t in range(TILES):
            rows = pl.ds(t * TILE, TILE)
            pre[rows, columns] = nn(edges[rows, :], weights[0:WIDTH])
        lifted[0:NODES, columns] = nn(nodes[...], weights[WIDTH : 2 * WIDTH]).astype(bf16)
        lifted[2 * NODES :, columns] = nn(nodes[...], weights[2 * WIDTH :]).astype(bf16)

    own_columns, other_columns = pl.ds(0, HALF), pl.ds(HALF, HALF)
    loads[0].wait()
    lift(first, own_columns)
    sent[0].wait_recv()
    lift(other_first, other_columns)
    sent[3].wait_recv()
    sent[4].wait_recv()
    for weights, columns in ((first, own_columns), (other_first, other_columns)):
        lifted[NODES : 2 * NODES, columns] = nn(
            table[NODES:], weights[WIDTH : 2 * WIDTH]
        ).astype(bf16)
    sent[1].wait_recv()
    sent[2].wait_recv()
    agg[...] = jnp.zeros_like(agg)

    def forward(t, _):
        rows = pl.ds(pl.multiple_of(t * TILE, TILE), TILE)
        chosen = hot[t]
        own = pre[rows, own_columns] + tn(chosen, lifted[:, own_columns]) + edge_bias[...]
        pre[rows, own_columns] = own
        own_act = silu(own).astype(bf16)
        act[rows, :] = own_act
        theirs = pre[rows, other_columns] + tn(chosen, lifted[:, other_columns]) + other_bias[...]
        out = nn(own_act, second[...]) + nn(silu(theirs).astype(bf16), other_second[...])
        values, scaled = normalize(out)
        normed[rows, :] = values
        scale[rows, :] = scaled
        agg[...] += nn(chosen[2 * NODES :], (edge_gain[...] * values).astype(bf16))
        return 0

    lax.fori_loop(0, TILES, forward, 0)
    node_input[0] = nodes[...]
    node_input[1] = agg[...].astype(bf16)
    for c in loads[1:4]:
        c.wait()
    node_pre = (
        nn(nodes[...], node_first[0:WIDTH]) + nn(node_input[1], node_first[WIDTH:]) + node_bias[...]
    )
    node_act[...] = silu(node_pre).astype(bf16)
    node_normed, node_scale = normalize(nn(node_act[...], node_second[...]))
    upstream = node_cot[...].astype(f32)
    sums[2:3] = jnp.sum(upstream * node_normed, axis=0, keepdims=True)
    node_dz = norm_back(upstream * node_gain[...], node_normed, node_scale).astype(bf16)
    node_dh = (nt(node_dz, node_second[...]) * silu_slope(node_pre)).astype(bf16)
    agg_grad[...] = nt(node_dh, node_first[WIDTH:]).astype(bf16)
    sums[3:4] = jnp.sum(node_dh.astype(f32), axis=0, keepdims=True)
    half_at = pl.multiple_of(core * HALF, HALF)
    other_at = pl.multiple_of((1 - core) * HALF, HALF)
    table_mine[0:NODES] = node_cot[:, pl.ds(half_at, HALF)].astype(f32) + nt(
        node_dh, node_first[pl.ds(half_at, HALF), :]
    )
    g[1024:1536] = tn(node_input[core], node_dh).astype(bf16)
    g[1536:1792] = tn(node_act[:, pl.ds(half_at, HALF)], node_dz).astype(bf16)
    loads[4].wait()
    sums[0:2] = jnp.zeros((2, WIDTH), f32)

    def backward(t, _):
        rows = pl.ds(pl.multiple_of(t * TILE, TILE), TILE)
        pulled = cot[rows, :].astype(f32) + tn(hot[t, 2 * NODES :], agg_grad[...])
        values = normed[rows, :]
        sums[0:1] += jnp.sum(pulled * values, axis=0, keepdims=True)
        tile_dz = norm_back(pulled * edge_gain[...], values, scale[rows, :]).astype(bf16)
        dz[rows, :] = tile_dz
        tile_dh = (nt(tile_dz, second[...]) * silu_slope(pre[rows, own_columns])).astype(bf16)
        dh[rows, :] = tile_dh
        sums[1:2, own_columns] += jnp.sum(tile_dh.astype(f32), axis=0, keepdims=True)
        edge_mine[rows, :] = cot[rows, pl.ds(half_at, HALF)].astype(f32) + nt(
            tile_dh, first[pl.ds(half_at, HALF), :]
        )
        edge_send[rows, :] = nt(tile_dh, first[pl.ds(other_at, HALF), :]).astype(bf16)
        return 0

    lax.fori_loop(0, TILES, backward, 0)
    gathered = sum(nn(hot[t], dh[t * TILE : (t + 1) * TILE]) for t in range(TILES)).astype(bf16)
    from_sender, from_receiver = gathered[0 : 2 * NODES], gathered[2 * NODES :]
    for target, at in ((table_mine, half_at), (table_send, other_at)):
        table_part = nt(from_sender, first[pl.ds(WIDTH + at, HALF), :])
        top = table_part[0:NODES] + nt(from_receiver, first[pl.ds(2 * WIDTH + at, HALF), :])
        if target is table_mine:
            target[0:NODES] += top
        else:
            target[0:NODES] = top.astype(bf16)
        target[NODES:] = table_part[NODES:].astype(target.dtype)
    g[0:512, own_columns] = tn(edges[...], dh[...]).astype(bf16)
    sender_grad = tn(table[...], from_sender).astype(bf16)
    g[512:768, own_columns] = sender_grad[0:256]
    g[0:256, other_columns] = sender_grad[256:512]
    g[256:768, other_columns] = tn(nodes[...], from_receiver).astype(bf16)
    g[768:1024] = tn(act[...], dz[...]).astype(bf16)
    mine = sums[:, pl.ds(half_at, HALF)]
    g[1792:2048] = jnp.zeros((256, WIDTH), bf16)
    row = lax.broadcasted_iota(jnp.int32, (16, HALF), 0)
    g[1792:1808, own_columns] = jnp.where(
        row == 0, sums[1:2, own_columns], jnp.where(row == 1, mine[3:4], 0.0)
    ).astype(bf16)
    g[1792:1808, other_columns] = jnp.where(
        row == 0, mine[0:1], jnp.where(row == 1, mine[2:3], 0.0)
    ).astype(bf16)
    for c in sent:
        c.wait_send()


def layer_call(*operands):
    bf16, f32 = jnp.bfloat16, jnp.float32
    dma = pltpu.SemaphoreType.DMA
    vmem = pl.BlockSpec(memory_space=pltpu.VMEM)
    far = pl.BlockSpec(memory_space=pl.ANY)
    return pl.pallas_call(
        layer_kernel,
        out_shape=(
            jax.ShapeDtypeStruct((ROWS, WIDTH), bf16),
            jax.ShapeDtypeStruct((EDGES, HALF), f32),
            jax.ShapeDtypeStruct((EDGES, HALF), bf16),
            jax.ShapeDtypeStruct((2 * NODES, HALF), f32),
            jax.ShapeDtypeStruct((2 * NODES, HALF), bf16),
        ),
        in_specs=[vmem] * 10 + [far] * 5,
        out_specs=(vmem,) * 5,
        scratch_shapes=[
            pltpu.VMEM((EDGES, WIDTH), bf16),
            pltpu.VMEM((EDGES, WIDTH), bf16),
            pltpu.VMEM((NODES, WIDTH), bf16),
            pltpu.VMEM((2 * WIDTH, WIDTH), bf16),
            pltpu.VMEM((WIDTH, WIDTH), bf16),
            pltpu.VMEM((3 * WIDTH, HALF), bf16),
            pltpu.VMEM((HALF, WIDTH), bf16),
            pltpu.VMEM((1, HALF), f32),
            pltpu.VMEM((NODES, WIDTH), bf16),
            pltpu.VMEM((2 * NODES, WIDTH), bf16),
            pltpu.VMEM((TILES, 3 * NODES, TILE), bf16),
            pltpu.VMEM((EDGES, WIDTH), f32),
            pltpu.VMEM((3 * NODES, WIDTH), bf16),
            pltpu.VMEM((EDGES, HALF), bf16),
            pltpu.VMEM((EDGES, WIDTH), f32),
            pltpu.VMEM((EDGES, 1), f32),
            pltpu.VMEM((NODES, WIDTH), f32),
            pltpu.VMEM((2, NODES, WIDTH), bf16),
            pltpu.VMEM((NODES, WIDTH), bf16),
            pltpu.VMEM((NODES, WIDTH), bf16),
            pltpu.VMEM((EDGES, WIDTH), bf16),
            pltpu.VMEM((EDGES, HALF), bf16),
            pltpu.VMEM((8, WIDTH), f32),
            dma((5,)),
            dma((2, 5)),
        ],
        compiler_params=pltpu.CompilerParams(
            collective_id=0, has_side_effects=True, vmem_limit_bytes=40 * 2**20
        ),
        name="layer",
    )(*operands)


def reduce_kernel(
    g,
    listed,
    edge_mine,
    edge_send,
    table_mine,
    table_send,
    out,
    other,
    grad_nodes,
    grad_edges,
    edge_got,
    table_got,
    table_sum,
    leaving,
    arriving,
    held_wide,
    made_wide,
    kept_wide,
    held_narrow,
    made_narrow,
    kept_narrow,
    held_z,
    sems_wide,
    sems_narrow,
    sems_z,
    sems_out_z,
    sems_out_narrow,
    sems_out_wide,
    sems_core,
    sems_side,
):
    batch = lax.axis_index("batch")
    space = lax.axis_index("space")
    core = lax.axis_index("hidden")
    x = space // 16
    y = (space // 8) % 2 * 2 + batch
    z = space % 8

    def device(i, j, k):
        return (j % 2, (i * 2 + j // 2) * 8 + k, core)

    x_up, x_down = (device((x + k) % 4, y, z) for k in (1, 3))
    y_up, y_down = (device(x, (y + k) % 4, z) for k in (1, 3))
    z_peers = [device(x, y, (z + k) % 8) for k in range(1, 8)]
    _, partner, before, after = places()
    barrier = pltpu.get_barrier_semaphore()
    peers = [x_up, x_down, y_up, y_down, *z_peers, partner, before, after]
    for peer in peers:
        pl.semaphore_signal(barrier, inc=1, device_id=peer, device_id_type=MESH)
    pl.semaphore_wait(barrier, len(peers))

    side = [
        remote(table_send, table_got, sems_side, 0, partner),
        remote(edge_send, edge_got, sems_side, 1, partner),
    ]
    for c in side:
        c.start()
    along = ((x, x_up, x_down), (y, y_up, y_down))
    started = []
    for color in (0, 1):
        pos, ahead, behind = along[color]
        started.append(
            scatter_start(
                g, color * COLOR, WIDE, pos, ahead, behind, held_wide.at[color], sems_wide.at[color]
            )
        )
    side[0].wait_recv()
    table_sum[...] = table_mine[...] + table_got[...].astype(jnp.float32)
    leaving[...] = table_sum[NODES:].astype(jnp.bfloat16)
    side += [
        remote(leaving.at[pl.ds(0, HALO)], arriving.at[pl.ds(HALO, HALO)], sems_side, 2, before),
        remote(leaving.at[pl.ds(HALO, HALO)], arriving.at[pl.ds(0, HALO)], sems_side, 3, after),
    ]
    for c in side[2:]:
        c.start()
    side[1].wait_recv()
    grad_edges[...] = (edge_mine[...] + edge_got[...].astype(jnp.float32)).astype(jnp.bfloat16)
    for color in (0, 1):
        pos, ahead, behind = along[color]
        scatter_middle(
            g, color * COLOR, WIDE, pos, ahead, behind, held_wide.at[color],
            made_wide.at[color], sems_wide.at[color], started[color],
        )
    second = []
    for color in (0, 1):
        pos, ahead, behind = along[color]
        scatter_end(
            g, color * COLOR, WIDE, pos, held_wide.at[color], kept_wide.at[color], 0, started[color]
        )
        pos, ahead, behind = along[1 - color]
        second.append(
            scatter_start(
                kept_wide.at[color], 0, NARROW, pos, ahead, behind,
                held_narrow.at[color], sems_narrow.at[color],
            )
        )
    for c in side[2:]:
        c.wait_recv()
    grad_nodes[...] = (
        table_sum[0:NODES] + nn(hot_columns(listed[...], NODES), arriving[...])
    ).astype(jnp.bfloat16)
    for c in side:
        c.wait_send()
    for color in (0, 1):
        pos, ahead, behind = along[1 - color]
        scatter_middle(
            kept_wide.at[color], 0, NARROW, pos, ahead, behind, held_narrow.at[color],
            made_narrow.at[color], sems_narrow.at[color], second[color],
        )
    for color in (0, 1):
        pos, ahead, behind = along[1 - color]
        scatter_end(
            kept_wide.at[color], 0, NARROW, pos, held_narrow.at[color],
            kept_narrow, color * NARROW, second[color],
        )
    third = []
    for k in range(1, 8):
        c = remote(
            rows_at(kept_narrow, (z + k) % 8 * ZROWS, ZROWS), held_z.at[k - 1], sems_z, k - 1,
            z_peers[k - 1],
        )
        c.start()
        third.append(c)
    total = load_rows(kept_narrow, z * ZROWS, ZROWS)
    for k in range(7):
        third[k].wait_recv()
        total = total + held_z[k].astype(jnp.float32)
    base = (x * WIDE + y * NARROW, COLOR + y * WIDE + x * NARROW)
    upper = z // 4
    mine = (1 - upper) * base[0] + upper * base[1] + z % 4 * ZROWS
    out[pl.ds(pl.multiple_of(mine, 16), ZROWS), :] = total.astype(jnp.bfloat16)
    for c in third:
        c.wait_send()
    third = []
    for k in range(1, 8):
        c = remote(rows_at(out, mine, ZROWS), rows_at(out, mine, ZROWS), sems_out_z, k - 1, z_peers[k - 1])
        c.start()
        third.append(c)
    for c in third:
        c.wait_recv()
    for c in third:
        c.wait_send()
    bases = ((0 + x * WIDE), (COLOR + y * WIDE))
    copies = []
    for color in (0, 1):
        pos, ahead, behind = along[1 - color]
        copies.append(gather_start(out, bases[color], NARROW, pos, ahead, behind, sems_out_narrow.at[color]))
    for color in (0, 1):
        pos, ahead, behind = along[1 - color]
        gather_middle(out, bases[color], NARROW, pos, ahead, behind, sems_out_narrow.at[color], copies[color])
    wide = []
    for color in (0, 1):
        gather_end(copies[color])
        pos, ahead, behind = along[color]
        wide.append(gather_start(out, color * COLOR, WIDE, pos, ahead, behind, sems_out_wide.at[color]))
    for color in (0, 1):
        pos, ahead, behind = along[color]
        gather_middle(out, color * COLOR, WIDE, pos, ahead, behind, sems_out_wide.at[color], wide[color])
    for color in (1, 0):
        gather_end(wide[color])
        if color == 1:
            c = remote(out.at[pl.ds(NODE_AT, NODE_ROWS)], other, sems_core, 0, partner)
            c.start()
    c.wait()


def reduce_call(packed, listed, edge_mine, edge_send, table_mine, table_send):
    dma = pltpu.SemaphoreType.DMA
    bf16, f32 = jnp.bfloat16, jnp.float32
    columns = packed.shape[1]
    vmem = pl.BlockSpec(memory_space=pltpu.VMEM)
    return pl.pallas_call(
        reduce_kernel,
        out_shape=(
            jax.ShapeDtypeStruct(packed.shape, bf16),
            jax.ShapeDtypeStruct((NODE_ROWS, columns), bf16),
            jax.ShapeDtypeStruct((NODES, HALF), bf16),
            jax.ShapeDtypeStruct((EDGES, HALF), bf16),
        ),
        in_specs=[vmem] * 6,
        out_specs=(vmem,) * 4,
        scratch_shapes=[
            pltpu.VMEM((EDGES, HALF), bf16),
            pltpu.VMEM((2 * NODES, HALF), bf16),
            pltpu.VMEM((2 * NODES, HALF), f32),
            pltpu.VMEM((NODES, HALF), bf16),
            pltpu.VMEM((NODES, HALF), bf16),
            pltpu.VMEM((2, 6, WIDE // 2, columns), bf16),
            pltpu.VMEM((2, 2, WIDE // 2, columns), bf16),
            pltpu.VMEM((2, WIDE, columns), bf16),
            pltpu.VMEM((2, 6, NARROW // 2, columns), bf16),
            pltpu.VMEM((2, 2, NARROW // 2, columns), bf16),
            pltpu.VMEM((2 * NARROW, columns), bf16),
            pltpu.VMEM((7, ZROWS, columns), bf16),
            dma((2, 2, 6)),
            dma((2, 2, 6)),
            dma((2, 7)),
            dma((2, 7)),
            dma((2, 2, 6)),
            dma((2, 2, 6)),
            dma((2, 1)),
            dma((2, 4)),
        ],
        compiler_params=pltpu.CompilerParams(
            collective_id=1, has_side_effects=True, vmem_limit_bytes=32 * 2**20
        ),
        name="reduce_all",
    )(packed, listed, edge_mine, edge_send, table_mine, table_send)


def unpack_kernel(
    summed, other, edge_first, edge_bias, edge_second, edge_gain, node_first, node_bias,
    node_second, node_gain,
):
    f32 = jnp.float32
    core = lax.axis_index("hidden")
    edge_first[0:768] = summed[0:768, 0:HALF].astype(f32)
    edge_first[768:1536] = summed[0:768, HALF:].astype(f32)
    edge_second[...] = summed[768:1024].astype(f32)
    small = summed[1792:1808].astype(f32)
    far_small = other[768:784].astype(f32)
    edge_bias[...] = small[0:1, 0:HALF]
    for rows, at, source, values in (
        (core, 1024, summed, small),
        (1 - core, 0, other, far_small),
    ):
        node_first[pl.ds(pl.multiple_of(rows * 512, 512), 512), :] = source[at : at + 512].astype(f32)
        node_second[pl.ds(pl.multiple_of(rows * 256, 256), 256), :] = source[
            at + 512 : at + 768
        ].astype(f32)
        columns = pl.ds(pl.multiple_of(rows * HALF, HALF), HALF)
        edge_gain[:, columns] = values[0:1, HALF:]
        node_bias[:, columns] = values[1:2, 0:HALF]
        node_gain[:, columns] = values[1:2, HALF:]


def unpack_call(summed, other):
    f32 = jnp.float32
    vmem = pl.BlockSpec(memory_space=pltpu.VMEM)
    shapes = ((1536, 256), (1, 256), (256, 512), (1, 512), (1024, 512), (1, 512), (512, 512), (1, 512))
    return pl.pallas_call(
        unpack_kernel,
        out_shape=tuple(jax.ShapeDtypeStruct(shape, f32) for shape in shapes),
        in_specs=[vmem] * 2,
        out_specs=(vmem,) * 8,
        compiler_params=pltpu.CompilerParams(vmem_limit_bytes=32 * 2**20),
        name="unpack",
    )(summed, other)


def on_device(
    nodes,
    edges,
    node_cotangent,
    edge_cotangent,
    senders,
    receivers,
    send_lists,
    edge_first,
    edge_bias,
    edge_second,
    edge_gain,
    node_first,
    node_bias,
    node_second,
    node_gain,
):
    listed = send_lists.reshape(1, -1)
    packed, edge_mine, edge_send, table_mine, table_send = layer_call(
        nodes[0],
        listed,
        senders[None],
        receivers[None],
        edge_first,
        edge_second,
        edge_bias[None],
        edge_gain[None],
        node_bias[None],
        node_gain[None],
        edges[0],
        edge_cotangent[0],
        node_cotangent[0],
        node_first,
        node_second,
    )
    summed, other, grad_nodes, grad_edges = reduce_call(
        packed, listed, edge_mine, edge_send, table_mine, table_send
    )
    first, bias, second, gain, n_first, n_bias, n_second, n_gain = unpack_call(summed, other)
    return (
        grad_nodes[None],
        grad_edges[None],
        first,
        bias[0],
        second,
        gain[0],
        n_first,
        n_bias[0],
        n_second,
        n_gain[0],
    )


def solution(mesh):
    placed = (
        P("batch", "space", None),
        P("batch", "space", None),
        P("batch", "space", None),
        P("batch", "space", None),
        P("space"),
        P("space"),
        P("space", None, None),
        P(None, "hidden"),
        P("hidden"),
        P("hidden", None),
        P(),
        P(),
        P(),
        P(),
        P(),
    )
    return jax.shard_map(
        on_device,
        mesh=mesh,
        in_specs=placed,
        out_specs=(
            P("batch", "space", "hidden"),
            P("batch", "space", "hidden"),
            P(None, "hidden"),
            P("hidden"),
            P("hidden", None),
            P(),
            P(),
            P(),
            P(),
            P(),
        ),
        check_vma=False,
    )
```
